128 devices in a mesh: row: 8 (over x, core), col: 16 (over z, y).
Axes of the slice: x: 4, y: 4, z: 4, core: 2. Of those that a mesh axis runs over, the one named last changes fastest.
Arguments:
- basis: bfloat16 [1152, 256, 128], P(('row', 'col')), may hold values from -1.5 to 1.5
- row_index: int32 [1152, 128], P(('row', 'col')), may hold values from 0 to 255
- group_slot: int32 [1152], P(('row', 'col')), may hold values from 0 to 1535, as said below
- x_blocks: bfloat16 [96, 256, 256], P('row', 'col')
- zinv_blocks: bfloat16 [96, 256, 256], P('row', 'col')
Outputs:
- schur_tiles: float32 [96, 2048, 2048], P('row', None, 'col')
The draws below stay inside these ranges and needn't reach their ends.
Inputs may be any that keep to these rules, and one draw needn't show every extreme that they name: Values are distinct; group_slot // 16 is the group's PSD block and group_slot % 16 its position there. A group stored on the device at (row index a, col index c) has its position among c * 1 to c + 1 - 1. Of the groups of one device, at most 2 belong to blocks of one index of row (blocks b with b // 12 equal to it), and every device reaches 2 for some index. The positions that the blocks of one index of row have on one index of col hold exactly 9 groups.
All inputs are finite; a program needn't handle non-finite values.
Results may differ from the reference program's by a relative error of at most 0.00048.
Values may be sent and summed in bfloat16 or wider, within the bound.
A program may use at most 192 MiB of HBM per device.

```python
import math
import jax
import jax.numpy as jnp
from jax import lax

N = 256
C = 128
GMAX = 16
BLK_ROW = 12
POS_DEV = 1
GRP_DEV = 9
NBLK = 96
NGRP = 1152
N_ROW = 8
N_COL = 16


def definite_blocks(key):
    key_off, key_lift = jax.random.split(key)
    spread = jax.random.uniform(key_off, (NBLK, N, N), jnp.float32, -4.0 / N, 4.0 / N)
    lift = jnp.exp(jax.random.uniform(key_lift, (NBLK, N), jnp.float32, math.log(0.5), math.log(2.0)))
    identity = jnp.eye(N, dtype=jnp.float32)
    spread = 0.5 * (spread + jnp.swapaxes(spread, 1, 2))
    spread = spread * (1.0 - identity)
    diagonal = jnp.sum(jnp.abs(spread), axis=2) + lift
    return (spread + diagonal[:, :, None] * identity).astype(jnp.bfloat16)


def draw_x_blocks(key, part):
    return definite_blocks(jax.random.fold_in(key, 11))


def draw_zinv_blocks(key, part):
    return definite_blocks(jax.random.fold_in(key, 23))


def permute_count(one_key, count):
    order = jax.random.permutation(one_key, count).astype(jnp.int32)
    serial = jnp.arange(count, dtype=jnp.int32)
    score = jnp.where(order == count - 1, -2, jnp.where(order == 0, -1, serial))
    return order[jnp.argsort(score, stable=True)]


def draw_group_slot(key, part):
    places = BLK_ROW * POS_DEV
    key_recv, key_home = jax.random.split(jax.random.fold_in(key, 7))
    recv_keys = jax.random.split(key_recv, N_ROW * N_COL)
    recv_perm = jax.vmap(lambda one_key: permute_count(one_key, places))(recv_keys).reshape(N_ROW, N_COL, places).astype(jnp.int32)
    home_keys = jax.random.split(key_home, N_ROW * N_COL)
    home_perm = jax.vmap(lambda one_key: jax.random.permutation(one_key, GRP_DEV))(home_keys).reshape(N_ROW, N_COL, GRP_DEV).astype(jnp.int32)
    home_row = jnp.arange(N_ROW, dtype=jnp.int32)
    offset = (home_row[:, None] - home_row[None, :]) % N_ROW
    counts = (GRP_DEV - offset + N_ROW - 1) // N_ROW
    before = jnp.cumsum(counts, axis=1) - counts
    serial = jnp.arange(GRP_DEV, dtype=jnp.int32)
    owner_at = (home_row[:, None] + serial[None, :]) % N_ROW
    rounds = serial // N_ROW
    arrival = before[owner_at, home_row[:, None]] + rounds[None, :]
    col_ids = jnp.arange(N_COL, dtype=jnp.int32)
    local_spot = recv_perm[owner_at[:, None, :], col_ids[None, :, None], arrival[:, None, :]]
    block_id = owner_at[:, None, :] * BLK_ROW + local_spot // POS_DEV
    position = col_ids[None, :, None] * POS_DEV + local_spot % POS_DEV
    slot_id = block_id * GMAX + position
    ordered = jnp.take_along_axis(slot_id, home_perm, axis=2)
    return ordered.reshape(-1).astype(jnp.int32)


def touch_ends(result, stream_key, least, largest):
    index_at = [jax.random.randint(jax.random.fold_in(stream_key, axis), (), 0, length) for axis, length in enumerate(result.shape)]
    longest = result.shape.index(max(result.shape))
    next_to = index_at[:longest] + [(index_at[longest] + 1) % result.shape[longest]] + index_at[longest + 1:]
    return result.at[tuple(index_at)].set(least).at[tuple(next_to)].set(largest)


def steps_of(rng, extent, cuts, least, top_value):
    def one(axis_at, blocks):
        steps = jax.random.uniform(jax.random.fold_in(jax.random.fold_in(rng, 6), axis_at), (blocks,), jnp.float32, least / len(cuts), top_value / len(cuts))
        return jnp.repeat(jnp.exp(steps), extent[axis_at] // blocks).reshape((-1,) + (1,) * (len(extent) - axis_at - 1))

    loudness = one(*cuts[0])
    for cut in cuts[1:]:
        loudness = loudness * one(*cut)
    return loudness


def gaussian(key, dims, scale, reach, pieces=(), kind=jnp.bfloat16):
    values = jax.random.normal(key, dims, jnp.float32) * scale
    if len(pieces) > 0:
        values = steps_of(key, dims, pieces, -0.22, 0.18) * values
    return jnp.clip(values, min=-reach, max=reach).astype(kind)


def setup_inputs(seed: int = 0) -> dict:
    key_of = jax.random.split(jax.random.key(seed), 6)
    return {
        "basis": gaussian(key_of[0], (NGRP, N, C), 0.25, 1.5, ((0, 128),)),
        "row_index": touch_ends(jax.random.randint(key_of[1], (NGRP, C), 0, N), jax.random.fold_in(key_of[1], 1), 0, N - 1).astype(jnp.int32),
        "group_slot": draw_group_slot(jax.random.fold_in(key_of[5], 71), 0),
        "x_blocks": draw_x_blocks(jax.random.fold_in(key_of[5], 71), 0),
        "zinv_blocks": draw_zinv_blocks(jax.random.fold_in(key_of[5], 71), 0),
    }


def tile_block(members):
    basis_block, rows_block, mask_block, x_block, z_block = members
    basis_wide = basis_block.astype(jnp.float32)
    image_x = jnp.einsum("pnc,nm->pcm", basis_wide, x_block.astype(jnp.float32), precision=lax.Precision.HIGHEST).astype(jnp.bfloat16)
    image_z = jnp.einsum("pnc,nm->pcm", basis_wide, z_block.astype(jnp.float32), precision=lax.Precision.HIGHEST).astype(jnp.bfloat16)
    x_rows = jnp.take(x_block, rows_block, axis=0)
    z_rows = jnp.take(z_block, rows_block, axis=0)
    stacked = jnp.concatenate([image_x, x_rows, image_z, z_rows], axis=1)
    products = jnp.einsum("pcn,qnk->pcqk", stacked.astype(jnp.float32), basis_wide, precision=lax.Precision.HIGHEST)
    products = products.reshape(GMAX, 4 * C, GMAX * C)
    picked = jnp.take(stacked, rows_block.reshape(-1), axis=2).astype(jnp.float32)
    tile_sum = products[:, C:2 * C] * picked[:, 2 * C:3 * C] + picked[:, C:2 * C] * products[:, 2 * C:3 * C]
    tile_sum = tile_sum + products[:, :C] * picked[:, 3 * C:] + picked[:, :C] * products[:, 3 * C:]
    column_mask = jnp.repeat(mask_block, C)
    tile_sum = tile_sum * mask_block[:, None, None] * column_mask[None, None, :]
    return tile_sum.reshape(GMAX * C, GMAX * C)


def reference(basis, row_index, group_slot, x_blocks, zinv_blocks):
    slot_total = NBLK * GMAX
    placed = jnp.zeros((slot_total, N, C), jnp.bfloat16).at[group_slot].set(basis).reshape(NBLK, GMAX, N, C)
    placed_rows = jnp.zeros((slot_total, C), jnp.int32).at[group_slot].set(row_index).reshape(NBLK, GMAX, C)
    present = jnp.zeros((slot_total,), jnp.float32).at[group_slot].set(1.0).reshape(NBLK, GMAX)
    return lax.map(tile_block, (placed, placed_rows, present, x_blocks, zinv_blocks))
```

```python
import jax
import jax.numpy as jnp
from jax import lax
from jax.experimental import pallas as pl
from jax.experimental.pallas import tpu as pltpu
from jax.sharding import PartitionSpec as P

bf16, f32, i32 = jnp.bfloat16, jnp.float32, jnp.int32
N, C, GMAX = 256, 128, 16
ROWS, COLS, SIDE = 8, 16, 4
OWNED, GROUPS, PAIR = 12, 9, 2
SLAB = N // COLS
CLASS_ROWS = C // 2
HALF_ROWS = CLASS_ROWS // 2
WHOLE = None
BATCHES = (
    ((0, 0), (1, 0), (3, 0), (0, 1)),
    ((0, 3), (2, 0), (0, 2), (1, 1)),
    ((1, 3), (3, 1), (3, 3)),
    ((2, 1), (1, 2)),
    ((2, 3), (3, 2), (2, 2)),
)
UNROLL = 3


def col_of(y, z):
    return z * SIDE + y


def one_hot_rows(rows):
    column = jnp.broadcast_to(rows, (C, C)).T
    lanes = lax.broadcasted_iota(i32, (C, C), 1)
    both = jnp.concatenate([column == lanes, column == lanes + C], axis=1)
    return jnp.where(both, 1.0, 0.0).astype(bf16)


def row_at(table, at):
    down = lax.broadcasted_iota(i32, table.shape, 0)
    return jnp.sum(jnp.where(down == at, table, 0), axis=0, keepdims=True)


def tiles_of(parts, x, z, q):
    stack = jnp.concatenate([a for ut, rows in parts for a in (ut, one_hot_rows(rows))], axis=0)
    sx = jnp.dot(stack, x, preferred_element_type=f32).astype(bf16)
    sz = jnp.dot(stack, z, preferred_element_type=f32).astype(bf16)
    tx = jnp.dot(sx, q, preferred_element_type=f32)
    tz = jnp.dot(sz, q, preferred_element_type=f32)
    out = []
    for i in range(len(parts)):
        lo, mid, hi = 2 * C * i, 2 * C * i + C, 2 * C * i + 2 * C
        su0, se0, su1, se1 = tx[lo:mid, :C], tx[lo:mid, C:], tx[mid:hi, :C], tx[mid:hi, C:]
        su2, se2, su3, se3 = tz[lo:mid, :C], tz[lo:mid, C:], tz[mid:hi, :C], tz[mid:hi, C:]
        out.append(su1 * se2 + se1 * su2 + su0 * se3 + se0 * su3)
    return out


def gather_kernel(
    slot_ref, basis_ref, rows_ref, x_ref, z_ref, tiles_ref, block_ref,
    send_ut, got_ut, send_meta, got_meta, all_meta, small_got, small_all,
    x_full, z_full, q_all, *rest,
):
    u_bufs = rest[:16]
    (xz_send, xz_recv, u_send, u_recv, a_send, a_recv, m_send, m_recv, b_send, b_recv, local) = rest[16:]
    my_row, my_col = lax.axis_index("row"), lax.axis_index("col")
    my_y, my_z = lax.rem(my_col, SIDE), my_col // SIDE

    row_peers = [lax.rem(my_row + d, ROWS) for d in range(1, ROWS)]
    col_peers = [lax.rem(my_col + d, COLS) for d in range(1, COLS)]
    barrier = pltpu.get_barrier_semaphore()
    for r in row_peers:
        pl.semaphore_signal(barrier, inc=1, device_id={"row": r})
    for c in col_peers:
        pl.semaphore_signal(barrier, inc=1, device_id={"col": c})

    def source_col(oy, oz):
        return col_of(lax.rem(my_y + SIDE - oy, SIDE), lax.rem(my_z + SIDE - oz, SIDE))

    def yz(cls, off):
        return off if cls == 0 else (off[1], off[0])

    def moved(off, dim, sign):
        new = list(off)
        new[dim] = (new[dim] + sign) % SIDE
        return tuple(new)

    def neighbour(cls, dim, sign):
        along_y = (dim == 0) == (cls == 0)
        y = lax.rem(my_y + SIDE + sign, SIDE) if along_y else my_y
        z = my_z if along_y else lax.rem(my_z + SIDE + sign, SIDE)
        return {"col": col_of(y, z)}

    def sem_at(cls, off, half):
        return cls * 32 + (off[0] * SIDE + off[1]) * 2 + (half or 0)

    def xz_region(cls, off, half):
        at = pl.ds(pl.multiple_of(source_col(*yz(cls, off)) * SLAB, SLAB), SLAB)
        full = x_full if cls == 0 else z_full
        if half is WHOLE:
            return full.at[:, at, :]
        return full.at[pl.ds(half * (OWNED // 2), OWNED // 2), at, :]

    def u_region(cls, off, half):
        oy, oz = yz(cls, off)
        buf = u_bufs[oy * SIDE + oz]
        if half is WHOLE:
            return buf.at[:, pl.ds(cls * CLASS_ROWS, CLASS_ROWS), :]
        return buf.at[:, pl.ds(cls * CLASS_ROWS + half * HALF_ROWS, HALF_ROWS), :]

    class Tree:
        def __init__(self, region, send_sems, recv_sems, same_place):
            self.region, self.send_sems, self.recv_sems = region, send_sems, recv_sems
            self.same_place, self.sent = same_place, []

        def copy(self, cls, off, dim, sign, half, source=None):
            there = moved(off, dim, sign)
            at = sem_at(cls, there, half)
            here = self.region(cls, off, half)
            copy = pltpu.make_async_remote_copy(
                src_ref=here if source is None else source,
                dst_ref=here if self.same_place else self.region(cls, there, half),
                send_sem=self.send_sems.at[at],
                recv_sem=self.recv_sems.at[at],
                device_id=neighbour(cls, dim, sign),
            )
            copy.start()
            self.sent.append(copy)

        def arrived(self, cls, off, half=WHOLE):
            at = sem_at(cls, off, half)
            here = self.region(cls, off, half)
            pltpu.make_async_remote_copy(
                src_ref=here, dst_ref=here,
                send_sem=self.send_sems.at[at], recv_sem=self.recv_sems.at[at],
                device_id=neighbour(cls, 0, 1),
            ).wait_recv()

        def first(self, sources=(None, None)):
            for dim in (0, 1):
                for sign in (1, -1):
                    for cls in (0, 1):
                        self.copy(cls, (0, 0), dim, sign, WHOLE, sources[cls])

        def near(self):
            for sign, off in ((1, 1), (-1, 3)):
                for cls in (0, 1):
                    self.arrived(cls, (off, 0))
                    self.copy(cls, (off, 0), 0, sign, 0 if sign > 0 else 1)
            for off in (1, 3):
                for cls in (0, 1):
                    for sign in (1, -1):
                        self.copy(cls, (off, 0), 1, sign, WHOLE)
            self.onward(0)

        def onward(self, unit):
            for sign, off in ((1, 1), (-1, 3)):
                for cls in (0, 1):
                    self.arrived(cls, (unit, off))
                    self.copy(cls, (unit, off), 1, sign, 0 if sign > 0 else 1)

        def opposite(self):
            for cls in (0, 1):
                for half in (0, 1):
                    self.arrived(cls, (2, 0), half)
                for sign in (1, -1):
                    self.copy(cls, (2, 0), 1, sign, WHOLE)

        def last(self, unit):
            for cls in (0, 1):
                for half in (0, 1):
                    self.arrived(cls, (unit, 2), half)

        def drain(self):
            for copy in self.sent:
                copy.wait_send()

    xz = Tree(xz_region, xz_send, xz_recv, True)
    ut = Tree(u_region, u_send, u_recv, False)

    lane = lax.broadcasted_iota(i32, (1, C), 1)
    slots = [slot_ref[g] for g in range(GROUPS)]
    blocks = [lax.div(s, GMAX) for s in slots]
    owners = [lax.div(b, OWNED) for b in blocks]
    targets = []
    for g in range(GROUPS):
        earlier = sum([(owners[h] == owners[g]).astype(i32) for h in range(g)], jnp.int32(0))
        targets.append(owners[g] * PAIR + earlier)
    for r in range(ROWS):
        note = jnp.zeros((1, C), i32)
        send_meta[r] = jnp.zeros((8, C), i32)
        for j in range(PAIR):
            t = r * PAIR + j
            src, code = jnp.int32(0), jnp.int32(0)
            for g in range(GROUPS):
                hit = targets[g] == t
                src = jnp.where(hit, g, src)
                code = jnp.where(hit, blocks[g] - owners[g] * OWNED + 1, code)
            note = jnp.where(lane == j, code, note)
            send_ut[t] = basis_ref[src].T
            rows = jnp.zeros((1, C), i32)
            for g in range(GROUPS):
                rows = jnp.where(jnp.full((1, C), targets[g]) == t, rows_ref[pl.ds(g, 1), :], rows)
            send_meta[r, pl.ds(j, 1), :] = rows
        send_meta[r, pl.ds(PAIR, 1), :] = note
    mine = pl.ds(pl.multiple_of(my_col * SLAB, SLAB), SLAB)
    x_full[:, mine, :] = x_ref[...]
    z_full[:, mine, :] = z_ref[...]
    for j in range(PAIR):
        got_ut[my_row * PAIR + j] = send_ut[my_row * PAIR + j]
    got_meta[my_row] = send_meta[my_row]

    pl.semaphore_wait(barrier, ROWS - 1 + COLS - 1)
    xz.first((x_ref, z_ref))

    def part(ref, r):
        many = ref.shape[0] // ROWS
        return ref.at[pl.ds(r * many, many)]

    def exchange(d, r, source, dest, sends, recvs):
        return pltpu.make_async_remote_copy(
            src_ref=part(source, r), dst_ref=part(dest, my_row),
            send_sem=sends.at[d], recv_sem=recvs.at[d], device_id={"row": r},
        )

    def from_row(d, dest, sends, recvs):
        r = lax.rem(my_row + ROWS - d, ROWS)
        return pltpu.make_async_remote_copy(
            src_ref=part(dest, r), dst_ref=part(dest, r),
            send_sem=sends.at[d], recv_sem=recvs.at[d], device_id={"row": r},
        )

    a_sent, m_sent, b_sent = [], [], []
    for d, r in zip(range(1, ROWS), row_peers):
        m_sent.append(exchange(d, r, send_meta, got_meta, m_send, m_recv))
        m_sent[-1].start()
    for d, r in zip(range(1, ROWS), row_peers):
        a_sent.append(exchange(d, r, send_ut, got_ut, a_send, a_recv))
        a_sent[-1].start()

    for d in range(1, ROWS):
        from_row(d, got_meta, m_send, m_recv).wait_recv()
    note_copy = pltpu.make_async_copy(got_meta, small_got, local.at[0])
    note_copy.start()
    note_copy.wait()
    codes = [small_got[t // PAIR, PAIR, t % PAIR] for t in range(ROWS * PAIR)]
    picks = [jnp.int32(0)] * GROUPS
    kept = [jnp.int32(0)] * GROUPS
    count = jnp.int32(0)
    for t in range(ROWS * PAIR):
        for k in range(GROUPS):
            hit = (codes[t] > 0) & (count == k)
            picks[k] = jnp.where(hit, t, picks[k])
            kept[k] = jnp.where(hit, codes[t] - 1, kept[k])
        count = count + (codes[t] > 0).astype(i32)
    table = jnp.full((1, C), 16, i32)
    for k in range(GROUPS):
        table = jnp.where(lane == kept[k], k, table)
    for k in range(GROUPS):
        table = jnp.where(lane == GMAX + k, kept[k], table)
        block_ref[k] = kept[k]
    all_meta[my_col] = jnp.zeros((GMAX, C), i32)
    for k in range(GROUPS):
        rows = jnp.zeros((1, C), i32)
        for t in range(ROWS * PAIR):
            rows = jnp.where(jnp.full((1, C), picks[k]) == t, got_meta[t // PAIR, pl.ds(t % PAIR, 1), :], rows)
        all_meta[my_col, pl.ds(k, 1), :] = rows
    all_meta[my_col, pl.ds(GROUPS, 1), :] = table

    xz.near()

    for d, c in zip(range(1, COLS), col_peers):
        b_sent.append(
            pltpu.make_async_remote_copy(
                src_ref=all_meta.at[my_col], dst_ref=all_meta.at[my_col],
                send_sem=b_send.at[d], recv_sem=b_recv.at[d], device_id={"col": c},
            )
        )
        b_sent[-1].start()

    xz.opposite()
    xz.onward(1)
    xz.onward(3)

    for d in range(1, ROWS):
        from_row(d, got_ut, a_send, a_recv).wait_recv()
    own = u_bufs[0]
    for k in range(GROUPS):
        own[k] = got_ut[picks[k]]

    xz.onward(2)
    ut.first()

    down = lax.broadcasted_iota(i32, (N, C), 0)
    for k in range(GROUPS):
        q_all[k, :, :C] = own[k].T
        q_all[k, :, C:] = jnp.where(down == all_meta[my_col, pl.ds(k, 1), :], 1.0, 0.0).astype(bf16)

    for unit in range(SIDE):
        xz.last(unit)
    for d in range(1, COLS):
        c = lax.rem(my_col + COLS - d, COLS)
        pltpu.make_async_remote_copy(
            src_ref=all_meta.at[c], dst_ref=all_meta.at[c],
            send_sem=b_send.at[d], recv_sem=b_recv.at[d], device_id={"col": c},
        ).wait_recv()
    table_copy = pltpu.make_async_copy(all_meta.at[:, pl.ds(8, 8), :], small_all, local.at[1])
    table_copy.start()
    table_copy.wait()

    def compute(batch):
        cols = [source_col(*off) for off in batch]
        bufs = [u_bufs[oy * SIDE + oz] for oy, oz in batch]

        def step(i, carry):
            for j in range(UNROLL):
                k = i * UNROLL + j
                b = small_all[my_col, GROUPS - 8, GMAX + k]
                codes = [small_all[c, GROUPS - 8, b] for c in cols]
                at = [jnp.where(code < GROUPS, code, 0) for code in codes]
                parts = [
                    (buf[s], row_at(all_meta[c], s))
                    for buf, c, s in zip(bufs, cols, at)
                ]
                for c, code, tile in zip(cols, codes, tiles_of(parts, x_full[b], z_full[b], q_all[k])):
                    tiles_ref[k, pl.ds(pl.multiple_of(c * C, C), C), :] = jnp.where(
                        jnp.full((C, C), code) < GROUPS, tile, 0.0
                    )
            return carry

        lax.fori_loop(0, GROUPS // UNROLL, step, 0)

    ut.near()
    compute(BATCHES[0])
    ut.opposite()
    ut.onward(1)
    ut.last(0)
    compute(BATCHES[1])
    ut.onward(3)
    compute(BATCHES[2])
    ut.onward(2)
    ut.last(1)
    compute(BATCHES[3])
    ut.last(3)
    ut.last(2)
    compute(BATCHES[4])

    xz.drain()
    ut.drain()
    for copy in a_sent + m_sent + b_sent:
        copy.wait_send()


def place_kernel(block_ref, tiles_ref, out_ref, zeros, full_sem, zero_sem):
    zeros[...] = jnp.zeros_like(zeros)
    full = [
        pltpu.make_async_copy(tiles_ref.at[k], out_ref.at[block_ref[k]], full_sem.at[k])
        for k in range(GROUPS)
    ]
    for copy in full:
        copy.start()
    count = jnp.int32(0)
    absent = [jnp.int32(0)] * (OWNED - GROUPS)
    for b in range(OWNED):
        found = block_ref[0] == b
        for k in range(1, GROUPS):
            found = found | (block_ref[k] == b)
        for m in range(OWNED - GROUPS):
            absent[m] = jnp.where(jnp.logical_not(found) & (count == m), b, absent[m])
        count = count + jnp.where(found, 0, 1)
    empty = [
        pltpu.make_async_copy(zeros, out_ref.at[absent[m]], zero_sem.at[m])
        for m in range(OWNED - GROUPS)
    ]
    for copy in empty:
        copy.start()
    for copy in full + empty:
        copy.wait()


def body(basis, row_index, group_slot, x_blocks, zinv_blocks):
    vmem, smem, anywhere = (
        pl.BlockSpec(memory_space=pltpu.VMEM),
        pl.BlockSpec(memory_space=pltpu.SMEM),
        pl.BlockSpec(memory_space=pl.ANY),
    )
    dma = pltpu.SemaphoreType.DMA
    tiles, blocks = pl.pallas_call(
        gather_kernel,
        out_shape=(
            pltpu.VMEM((GROUPS, GMAX * C, C), f32),
            jax.ShapeDtypeStruct((GMAX,), i32),
        ),
        in_specs=[smem, vmem, vmem, vmem, vmem],
        out_specs=(vmem, smem),
        scratch_shapes=[
            pltpu.VMEM((ROWS * PAIR, C, N), bf16),
            pltpu.VMEM((ROWS * PAIR, C, N), bf16),
            pltpu.VMEM((ROWS, 8, C), i32),
            pltpu.VMEM((ROWS, 8, C), i32),
            pltpu.VMEM((COLS, GMAX, C), i32),
            pltpu.SMEM((ROWS, 8, C), i32),
            pltpu.SMEM((COLS, 8, C), i32),
            pltpu.VMEM((OWNED, N, N), bf16),
            pltpu.VMEM((OWNED, N, N), bf16),
            pltpu.VMEM((GROUPS, N, N), bf16),
        ]
        + [pltpu.VMEM((GROUPS, C, N), bf16)] * 16
        + [dma((64,))] * 4
        + [dma((ROWS,))] * 4
        + [dma((COLS,))] * 2
        + [dma((2,))],
        compiler_params=pltpu.CompilerParams(
            collective_id=0, has_side_effects=True, vmem_limit_bytes=44 << 20
        ),
        name="gather_tiles",
    )(group_slot, basis, row_index, x_blocks, zinv_blocks)
    return pl.pallas_call(
        place_kernel,
        out_shape=jax.ShapeDtypeStruct((OWNED, GMAX * C, C), f32),
        in_specs=[smem, vmem],
        out_specs=anywhere,
        scratch_shapes=[pltpu.VMEM((GMAX * C, C), f32), dma((GROUPS,)), dma((OWNED - GROUPS,))],
        compiler_params=pltpu.CompilerParams(vmem_limit_bytes=16 << 20),
        name="place_tiles",
    )(blocks, tiles)


def solution(mesh):
    placed = (
        P(("row", "col"), None, None),
        P(("row", "col"), None),
        P(("row", "col")),
        P("row", "col", None),
        P("row", "col", None),
    )
    return jax.shard_map(
        body, mesh=mesh, in_specs=placed, out_specs=P("row", None, "col"), check_vma=False
    )
```

```python
import jax
import jax.numpy as jnp
from jax import lax
from jax.experimental import pallas as pl
from jax.experimental.pallas import tpu as pltpu
from jax.sharding import PartitionSpec as P

bf16, f32, i32 = jnp.bfloat16, jnp.float32, jnp.int32
N, C, GMAX = 256, 128, 16
ROWS, COLS, SIDE = 8, 16, 4
OWNED, GROUPS, PAIR = 12, 9, 2
SLAB = N // COLS
CLASS_ROWS = C // 2
HALF_ROWS = CLASS_ROWS // 2
WHOLE = None
BATCHES = (
    ((0, 0), (1, 0), (3, 0), (0, 1)),
    ((0, 3), (1, 1)),
    ((1, 3), (3, 1), (3, 3)),
    ((2, 0), (0, 2)),
    ((2, 1), (1, 2)),
    ((2, 3), (3, 2)),
    ((2, 2),),
)
UNROLL = 3


def col_of(y, z):
    return z * SIDE + y


def one_hot_rows(rows):
    column = jnp.broadcast_to(rows, (C, C)).T
    lanes = lax.broadcasted_iota(i32, (C, C), 1)
    both = jnp.concatenate([column == lanes, column == lanes + C], axis=1)
    return jnp.where(both, 1.0, 0.0).astype(bf16)


def row_at(table, at):
    down = lax.broadcasted_iota(i32, table.shape, 0)
    return jnp.sum(jnp.where(down == at, table, 0), axis=0, keepdims=True)


def tiles_of(parts, x, z, q):
    stack = jnp.concatenate([a for ut, rows in parts for a in (ut, one_hot_rows(rows))], axis=0)
    sx = jnp.dot(stack, x, preferred_element_type=f32).astype(bf16)
    sz = jnp.dot(stack, z, preferred_element_type=f32).astype(bf16)
    tx = jnp.dot(sx, q, preferred_element_type=f32)
    tz = jnp.dot(sz, q, preferred_element_type=f32)
    out = []
    for i in range(len(parts)):
        lo, mid, hi = 2 * C * i, 2 * C * i + C, 2 * C * i + 2 * C
        su0, se0, su1, se1 = tx[lo:mid, :C], tx[lo:mid, C:], tx[mid:hi, :C], tx[mid:hi, C:]
        su2, se2, su3, se3 = tz[lo:mid, :C], tz[lo:mid, C:], tz[mid:hi, :C], tz[mid:hi, C:]
        out.append(su1 * se2 + se1 * su2 + su0 * se3 + se0 * su3)
    return out


def gather_kernel(
    slot_ref, basis_hbm, rows_hbm, x_ref, z_ref, tiles_ref, block_ref,
    basis_ref, rows_ref, send_ut, relay, got_ut, send_meta, got_meta, all_meta, small_got, small_all,
    x_full, z_full, q_all, *rest,
):
    u_bufs = rest[:16]
    (xz_send, xz_recv, u_send, u_recv, a_send, a_recv, m_send, m_recv, b_send, b_recv, local) = rest[16:]
    my_row, my_col = lax.axis_index("row"), lax.axis_index("col")
    my_y, my_z = lax.rem(my_col, SIDE), my_col // SIDE
    my_x, my_core = my_row // 2, lax.rem(my_row, 2)
    mine = pl.ds(pl.multiple_of(my_col * SLAB, SLAB), SLAB)
    loads = [
        pltpu.make_async_copy(source, dest, local.at[i])
        for i, (source, dest) in enumerate((
            (basis_hbm, basis_ref),
            (rows_hbm, rows_ref),
            (x_ref, x_full.at[:, mine, :]),
            (z_ref, z_full.at[:, mine, :]),
        ))
    ]
    for copy in loads:
        copy.start()

    row_peers = [lax.rem(my_row + d, ROWS) for d in range(1, ROWS)]
    y_peers = [col_of(lax.rem(my_y + d, SIDE), my_z) for d in range(1, SIDE)]
    z_peers = [col_of(my_y, lax.rem(my_z + d, SIDE)) for d in range(1, SIDE)]
    barrier = pltpu.get_barrier_semaphore()
    for r in row_peers:
        pl.semaphore_signal(barrier, inc=1, device_id={"row": r})
    for c in y_peers + z_peers:
        pl.semaphore_signal(barrier, inc=1, device_id={"col": c})

    def source_col(oy, oz):
        return col_of(lax.rem(my_y + SIDE - oy, SIDE), lax.rem(my_z + SIDE - oz, SIDE))

    def yz(cls, off):
        return off if cls == 0 else (off[1], off[0])

    def moved(off, dim, sign):
        new = list(off)
        new[dim] = (new[dim] + sign) % SIDE
        return tuple(new)

    def neighbour(cls, dim, sign):
        along_y = (dim == 0) == (cls == 0)
        y = lax.rem(my_y + SIDE + sign, SIDE) if along_y else my_y
        z = my_z if along_y else lax.rem(my_z + SIDE + sign, SIDE)
        return {"col": col_of(y, z)}

    def sem_at(cls, off, half):
        return cls * 32 + (off[0] * SIDE + off[1]) * 2 + (half or 0)

    def xz_region(cls, off, half):
        at = pl.ds(pl.multiple_of(source_col(*yz(cls, off)) * SLAB, SLAB), SLAB)
        full = x_full if cls == 0 else z_full
        if half is WHOLE:
            return full.at[:, at, :]
        return full.at[pl.ds(half * (OWNED // 2), OWNED // 2), at, :]

    def u_region(cls, off, half):
        oy, oz = yz(cls, off)
        buf = u_bufs[oy * SIDE + oz]
        if half is WHOLE:
            return buf.at[:, pl.ds(cls * CLASS_ROWS, CLASS_ROWS), :]
        return buf.at[:, pl.ds(cls * CLASS_ROWS + half * HALF_ROWS, HALF_ROWS), :]

    class Tree:
        def __init__(self, region, send_sems, recv_sems, same_place):
            self.region, self.send_sems, self.recv_sems = region, send_sems, recv_sems
            self.same_place, self.sent = same_place, []

        def copy(self, cls, off, dim, sign, half, source=None):
            there = moved(off, dim, sign)
            at = sem_at(cls, there, half)
            here = self.region(cls, off, half)
            copy = pltpu.make_async_remote_copy(
                src_ref=here if source is None else source,
                dst_ref=here if self.same_place else self.region(cls, there, half),
                send_sem=self.send_sems.at[at],
                recv_sem=self.recv_sems.at[at],
                device_id=neighbour(cls, dim, sign),
            )
            copy.start()
            self.sent.append(copy)

        def arrived(self, cls, off, half=WHOLE):
            at = sem_at(cls, off, half)
            here = self.region(cls, off, half)
            pltpu.make_async_remote_copy(
                src_ref=here, dst_ref=here,
                send_sem=self.send_sems.at[at], recv_sem=self.recv_sems.at[at],
                device_id=neighbour(cls, 0, 1),
            ).wait_recv()

        def first(self, sources=(None, None), dims=(0, 1)):
            for dim in dims:
                for sign in (1, -1):
                    for cls in (0, 1):
                        self.copy(cls, (0, 0), dim, sign, WHOLE, sources[cls])

        def near(self):
            self.spread()
            self.onward(0)

        def spread(self):
            for sign, off in ((1, 1), (-1, 3)):
                for cls in (0, 1):
                    self.arrived(cls, (off, 0))
                    self.copy(cls, (off, 0), 0, sign, 0 if sign > 0 else 1)
            for off in (1, 3):
                for cls in (0, 1):
                    for sign in (1, -1):
                        self.copy(cls, (off, 0), 1, sign, WHOLE)

        def onward(self, unit):
            for sign, off in ((1, 1), (-1, 3)):
                for cls in (0, 1):
                    self.arrived(cls, (unit, off))
                    self.copy(cls, (unit, off), 1, sign, 0 if sign > 0 else 1)

        def opposite(self):
            for cls in (0, 1):
                for half in (0, 1):
                    self.arrived(cls, (2, 0), half)
                for sign in (1, -1):
                    self.copy(cls, (2, 0), 1, sign, WHOLE)

        def last(self, unit):
            for cls in (0, 1):
                for half in (0, 1):
                    self.arrived(cls, (unit, 2), half)

        def drain(self):
            for copy in self.sent:
                copy.wait_send()

    xz = Tree(xz_region, xz_send, xz_recv, True)
    ut = Tree(u_region, u_send, u_recv, False)

    lane = lax.broadcasted_iota(i32, (1, C), 1)
    slots = [slot_ref[g] for g in range(GROUPS)]
    blocks = [lax.div(s, GMAX) for s in slots]
    owners = [lax.div(b, OWNED) for b in blocks]
    targets = []
    for g in range(GROUPS):
        earlier = sum([(owners[h] == owners[g]).astype(i32) for h in range(g)], jnp.int32(0))
        targets.append(owners[g] * PAIR + earlier)
    for copy in loads[:2]:
        copy.wait()
    for r in range(ROWS):
        note = jnp.zeros((1, C), i32)
        send_meta[r] = jnp.zeros((8, C), i32)
        for j in range(PAIR):
            t = r * PAIR + j
            src, code = jnp.int32(0), jnp.int32(0)
            for g in range(GROUPS):
                hit = targets[g] == t
                src = jnp.where(hit, g, src)
                code = jnp.where(hit, blocks[g] - owners[g] * OWNED + 1, code)
            note = jnp.where(lane == j, code, note)
            send_ut[r // 2, j, r % 2] = basis_ref[src].T
            rows = jnp.zeros((1, C), i32)
            for g in range(GROUPS):
                rows = jnp.where(jnp.full((1, C), targets[g]) == t, rows_ref[pl.ds(g, 1), :], rows)
            send_meta[r, pl.ds(j, 1), :] = rows
        send_meta[r, pl.ds(PAIR, 1), :] = note
    for j in range(PAIR):
        got_ut[my_row * PAIR + j] = send_ut[my_x, j, my_core]
    got_meta[my_row] = send_meta[my_row]

    pl.semaphore_wait(barrier, ROWS - 1 + 2 * (SIDE - 1))
    def exchange(d, r, sends, recvs):
        return pltpu.make_async_remote_copy(
            src_ref=send_meta.at[r], dst_ref=got_meta.at[my_row],
            send_sem=sends.at[d], recv_sem=recvs.at[d], device_id={"row": r},
        )

    def from_row(d, sends, recvs):
        r = lax.rem(my_row + ROWS - d, ROWS)
        return pltpu.make_async_remote_copy(
            src_ref=got_meta.at[r], dst_ref=got_meta.at[r],
            send_sem=sends.at[d], recv_sem=recvs.at[d], device_id={"row": r},
        )

    sides = [lax.rem(my_x + 1, SIDE), lax.rem(my_x + SIDE - 1, SIDE)]
    across = lax.rem(my_x + 2, SIDE)

    def to(source, dest, sem, x, core):
        return pltpu.make_async_remote_copy(
            src_ref=source, dst_ref=dest, send_sem=a_send.at[sem], recv_sem=a_recv.at[sem],
            device_id={"row": x * 2 + core},
        )

    def pair_of(row):
        return got_ut.at[pl.ds(row * PAIR, PAIR)]

    a_sent, m_sent, b_sent = [], [], []
    for i in range(2):
        a_sent.append(to(send_ut.at[across, i], relay.at[i], i, sides[i], my_core))
    for i in range(2):
        for same in range(2):
            core = lax.rem(my_core + same, 2)
            a_sent.append(to(send_ut.at[sides[i], :, core], pair_of(my_row), 2 + i * 2 + same, sides[i], core))
    other = lax.rem(my_core + 1, 2)
    a_sent.append(to(send_ut.at[my_x, :, other], pair_of(my_row), 6, my_x, other))

    for copy in a_sent[:2]:
        copy.start()
    for d, r in zip(range(1, ROWS), row_peers):
        m_sent.append(exchange(d, r, m_send, m_recv))
        m_sent[-1].start()
    xz.first((x_ref, z_ref))
    for copy in a_sent[2:]:
        copy.start()

    xz.spread()
    for i in range(2):
        to(relay.at[i], relay.at[i], i, sides[i], my_core).wait_recv()
        origin = sides[1 - i] * 2 + my_core
        for core in range(2):
            a_sent.append(
                to(relay.at[i, core], got_ut.at[origin * PAIR + i], 7 + i * 4 + core * 2 + my_core, sides[i], core)
            )
            a_sent[-1].start()
    xz.onward(0)

    for d in range(1, ROWS):
        from_row(d, m_send, m_recv).wait_recv()
    note_copy = pltpu.make_async_copy(got_meta, small_got, local.at[4])
    note_copy.start()
    note_copy.wait()
    codes = [small_got[t // PAIR, PAIR, t % PAIR] for t in range(ROWS * PAIR)]
    picks = [jnp.int32(0)] * GROUPS
    kept = [jnp.int32(0)] * GROUPS
    count = jnp.int32(0)
    for t in range(ROWS * PAIR):
        for k in range(GROUPS):
            hit = (codes[t] > 0) & (count == k)
            picks[k] = jnp.where(hit, t, picks[k])
            kept[k] = jnp.where(hit, codes[t] - 1, kept[k])
        count = count + (codes[t] > 0).astype(i32)
    table = jnp.full((1, C), 16, i32)
    for k in range(GROUPS):
        table = jnp.where(lane == kept[k], k, table)
    for k in range(GROUPS):
        table = jnp.where(lane == GMAX + k, kept[k], table)
        block_ref[k] = kept[k]
    all_meta[my_col] = jnp.zeros((GMAX, C), i32)
    for k in range(GROUPS):
        rows = jnp.zeros((1, C), i32)
        for t in range(ROWS * PAIR):
            rows = jnp.where(jnp.full((1, C), picks[k]) == t, got_meta[t // PAIR, pl.ds(t % PAIR, 1), :], rows)
        all_meta[my_col, pl.ds(k, 1), :] = rows
    all_meta[my_col, pl.ds(GROUPS, 1), :] = table

    def noted(at, sem, c):
        return pltpu.make_async_remote_copy(
            src_ref=at, dst_ref=at,
            send_sem=b_send.at[sem], recv_sem=b_recv.at[sem], device_id={"col": c},
        )

    def notes_of(z):
        return all_meta.at[pl.ds(z * SIDE, SIDE)]

    for d in range(1, SIDE):
        b_sent.append(noted(all_meta.at[my_col], d, y_peers[d - 1]))
        b_sent[-1].start()
    xz.opposite()
    for d in range(1, SIDE):
        c = col_of(lax.rem(my_y + SIDE - d, SIDE), my_z)
        noted(all_meta.at[c], d, c).wait_recv()
    for d in range(1, SIDE):
        b_sent.append(noted(notes_of(my_z), SIDE + d, z_peers[d - 1]))
        b_sent[-1].start()
    xz.onward(1)
    xz.onward(3)

    for i in range(2):
        for same in range(2):
            core = lax.rem(my_core + same, 2)
            dest = pair_of(sides[1 - i] * 2 + core)
            to(dest, dest, 2 + i * 2 + same, sides[i], core).wait_recv()
    dest = pair_of(my_x * 2 + other)
    to(dest, dest, 6, my_x, other).wait_recv()
    for i in range(2):
        for core in range(2):
            dest = got_ut.at[(across * 2 + core) * PAIR + i]
            sem = 7 + i * 4 + my_core * 2 + core
            to(dest, dest, sem, sides[i], core).wait_recv()
    own = u_bufs[0]
    for k in range(GROUPS):
        own[k] = got_ut[picks[k]]

    ut.first(dims=(0,))
    xz.onward(2)
    ut.first(dims=(1,))

    down = lax.broadcasted_iota(i32, (N, C), 0)
    for k in range(GROUPS):
        q_all[k, :, :C] = own[k].T
        q_all[k, :, C:] = jnp.where(down == all_meta[my_col, pl.ds(k, 1), :], 1.0, 0.0).astype(bf16)

    for unit in range(SIDE):
        xz.last(unit)
    for copy in loads[2:]:
        copy.wait()
    for d in range(1, SIDE):
        z = lax.rem(my_z + SIDE - d, SIDE)
        noted(notes_of(z), SIDE + d, col_of(my_y, z)).wait_recv()
    table_copy = pltpu.make_async_copy(all_meta.at[:, pl.ds(8, 8), :], small_all, local.at[5])
    table_copy.start()
    table_copy.wait()

    def compute(batch):
        cols = [source_col(*off) for off in batch]
        bufs = [u_bufs[oy * SIDE + oz] for oy, oz in batch]

        def step(i, carry):
            for j in range(UNROLL):
                k = i * UNROLL + j
                b = small_all[my_col, GROUPS - 8, GMAX + k]
                codes = [small_all[c, GROUPS - 8, b] for c in cols]
                at = [jnp.where(code < GROUPS, code, 0) for code in codes]
                parts = [
                    (buf[s], row_at(all_meta[c], s))
                    for buf, c, s in zip(bufs, cols, at)
                ]
                for c, code, tile in zip(cols, codes, tiles_of(parts, x_full[b], z_full[b], q_all[k])):
                    tiles_ref[k, pl.ds(pl.multiple_of(c * C, C), C), :] = jnp.where(
                        jnp.full((C, C), code) < GROUPS, tile, 0.0
                    )
            return carry

        lax.fori_loop(0, GROUPS // UNROLL, step, 0)

    ut.near()
    compute(BATCHES[0])
    ut.opposite()
    ut.onward(1)
    compute(BATCHES[1])
    ut.onward(3)
    compute(BATCHES[2])
    ut.last(0)
    compute(BATCHES[3])
    ut.onward(2)
    ut.last(1)
    compute(BATCHES[4])
    ut.last(3)
    compute(BATCHES[5])
    ut.last(2)
    compute(BATCHES[6])

    xz.drain()
    ut.drain()
    for copy in a_sent + m_sent + b_sent:
        copy.wait_send()


def place_kernel(block_ref, tiles_ref, out_ref, zeros, full_sem, zero_sem):
    zeros[...] = jnp.zeros_like(zeros)
    full = [
        pltpu.make_async_copy(tiles_ref.at[k], out_ref.at[block_ref[k]], full_sem.at[k])
        for k in range(GROUPS)
    ]
    for copy in full:
        copy.start()
    count = jnp.int32(0)
    absent = [jnp.int32(0)] * (OWNED - GROUPS)
    for b in range(OWNED):
        found = block_ref[0] == b
        for k in range(1, GROUPS):
            found = found | (block_ref[k] == b)
        for m in range(OWNED - GROUPS):
            absent[m] = jnp.where(jnp.logical_not(found) & (count == m), b, absent[m])
        count = count + jnp.where(found, 0, 1)
    empty = [
        pltpu.make_async_copy(zeros, out_ref.at[absent[m]], zero_sem.at[m])
        for m in range(OWNED - GROUPS)
    ]
    for copy in empty:
        copy.start()
    for copy in full + empty:
        copy.wait()


def body(basis, row_index, group_slot, x_blocks, zinv_blocks):
    hbm, vmem, smem, anywhere = (
        pl.BlockSpec(memory_space=pltpu.HBM),
        pl.BlockSpec(memory_space=pltpu.VMEM),
        pl.BlockSpec(memory_space=pltpu.SMEM),
        pl.BlockSpec(memory_space=pl.ANY),
    )
    dma = pltpu.SemaphoreType.DMA
    tiles, blocks = pl.pallas_call(
        gather_kernel,
        out_shape=(
            pltpu.VMEM((GROUPS, GMAX * C, C), f32),
            jax.ShapeDtypeStruct((GMAX,), i32),
        ),
        in_specs=[smem, hbm, hbm, hbm, hbm],
        out_specs=(vmem, smem),
        scratch_shapes=[
            pltpu.VMEM((GROUPS, N, C), bf16),
            pltpu.VMEM((GROUPS, C), i32),
            pltpu.VMEM((SIDE, PAIR, 2, C, N), bf16),
            pltpu.VMEM((2, 2, C, N), bf16),
            pltpu.VMEM((ROWS * PAIR, C, N), bf16),
            pltpu.VMEM((ROWS, 8, C), i32),
            pltpu.VMEM((ROWS, 8, C), i32),
            pltpu.VMEM((COLS, GMAX, C), i32),
            pltpu.SMEM((ROWS, 8, C), i32),
            pltpu.SMEM((COLS, 8, C), i32),
            pltpu.VMEM((OWNED, N, N), bf16),
            pltpu.VMEM((OWNED, N, N), bf16),
            pltpu.VMEM((GROUPS, N, N), bf16),
        ]
        + [pltpu.VMEM((GROUPS, C, N), bf16)] * 16
        + [dma((64,))] * 4
        + [dma((16,))] * 2
        + [dma((ROWS,))] * 2
        + [dma((2 * SIDE,))] * 2
        + [dma((6,))],
        compiler_params=pltpu.CompilerParams(
            collective_id=0, has_side_effects=True, vmem_limit_bytes=57_500_000
        ),
        name="gather_tiles",
    )(group_slot, basis, row_index, x_blocks, zinv_blocks)
    return pl.pallas_call(
        place_kernel,
        out_shape=jax.ShapeDtypeStruct((OWNED, GMAX * C, C), f32),
        in_specs=[smem, vmem],
        out_specs=anywhere,
        scratch_shapes=[pltpu.VMEM((GMAX * C, C), f32), dma((GROUPS,)), dma((OWNED - GROUPS,))],
        compiler_params=pltpu.CompilerParams(vmem_limit_bytes=16 << 20),
        name="place_tiles",
    )(blocks, tiles)


def solution(mesh):
    placed = (
        P(("row", "col"), None, None),
        P(("row", "col"), None),
        P(("row", "col")),
        P("row", "col", None),
        P("row", "col", None),
    )
    return jax.shard_map(
        body, mesh=mesh, in_specs=placed, out_specs=P("row", None, "col"), check_vma=False
    )
```

```python
import jax
import jax.numpy as jnp
from jax import lax
from jax.experimental import pallas as pl
from jax.experimental.pallas import tpu as pltpu
from jax.sharding import PartitionSpec as P

bf16, f32, i32 = jnp.bfloat16, jnp.float32, jnp.int32
N, C, GMAX = 256, 128, 16
ROWS, COLS, SIDE = 8, 16, 4
OWNED, GROUPS, PAIR = 12, 9, 2
SLAB = N // COLS
CLASS_ROWS = C // 2
HALF_ROWS = CLASS_ROWS // 2
WHOLE = None
BATCHES = (
    ((0, 0), (1, 0), (3, 0), (0, 1)),
    ((0, 3), (1, 1)),
    ((1, 3), (3, 1), (3, 3)),
    ((2, 0), (0, 2)),
)
LATE = ((2, 1), (1, 2), (2, 3), (3, 2), (2, 2))
UNROLL = 3


def col_of(y, z):
    return z * SIDE + y


def one_hot_rows(rows):
    column = jnp.broadcast_to(rows, (C, C)).T
    lanes = lax.broadcasted_iota(i32, (C, C), 1)
    both = jnp.concatenate([column == lanes, column == lanes + C], axis=1)
    return jnp.where(both, 1.0, 0.0).astype(bf16)


def row_at(table, at):
    down = lax.broadcasted_iota(i32, table.shape, 0)
    return jnp.sum(jnp.where(down == at, table, 0), axis=0, keepdims=True)


def tiles_of(parts, x, z, q):
    stack = jnp.concatenate([a for ut, rows in parts for a in (ut, one_hot_rows(rows))], axis=0)
    tx, tz = products_of(stack, x, z, q)
    out = []
    for i in range(len(parts)):
        lo, mid, hi = 2 * C * i, 2 * C * i + C, 2 * C * i + 2 * C
        su0, se0, su1, se1 = tx[lo:mid, :C], tx[lo:mid, C:], tx[mid:hi, :C], tx[mid:hi, C:]
        su2, se2, su3, se3 = tz[lo:mid, :C], tz[lo:mid, C:], tz[mid:hi, :C], tz[mid:hi, C:]
        out.append(su1 * se2 + se1 * su2 + su0 * se3 + se0 * su3)
    return out


def products_of(stack, x, z, q):
    sx = jnp.dot(stack, x, preferred_element_type=f32).astype(bf16)
    sz = jnp.dot(stack, z, preferred_element_type=f32).astype(bf16)
    return (
        jnp.dot(sx, q, preferred_element_type=f32),
        jnp.dot(sz, q, preferred_element_type=f32),
    )


def gather_kernel(
    slot_ref, basis_hbm, rows_hbm, x_ref, z_ref, tiles_ref, block_ref,
    basis_ref, rows_ref, send_ut, relay, got_ut, send_meta, got_meta, all_meta, small_got, small_all,
    x_full, z_full, q_all, ahead, *rest,
):
    u_bufs = rest[:16]
    (xz_send, xz_recv, u_send, u_recv, a_send, a_recv, m_send, m_recv, b_send, b_recv, local) = rest[16:]
    my_row, my_col = lax.axis_index("row"), lax.axis_index("col")
    my_y, my_z = lax.rem(my_col, SIDE), my_col // SIDE
    my_x, my_core = my_row // 2, lax.rem(my_row, 2)
    mine = pl.ds(pl.multiple_of(my_col * SLAB, SLAB), SLAB)
    loads = [
        pltpu.make_async_copy(source, dest, local.at[i])
        for i, (source, dest) in enumerate((
            (basis_hbm, basis_ref),
            (rows_hbm, rows_ref),
            (x_ref, x_full.at[:, mine, :]),
            (z_ref, z_full.at[:, mine, :]),
        ))
    ]
    for copy in loads:
        copy.start()

    row_peers = [lax.rem(my_row + d, ROWS) for d in range(1, ROWS)]
    y_peers = [col_of(lax.rem(my_y + d, SIDE), my_z) for d in range(1, SIDE)]
    z_peers = [col_of(my_y, lax.rem(my_z + d, SIDE)) for d in range(1, SIDE)]
    barrier = pltpu.get_barrier_semaphore()
    for r in row_peers:
        pl.semaphore_signal(barrier, inc=1, device_id={"row": r})
    for c in y_peers + z_peers:
        pl.semaphore_signal(barrier, inc=1, device_id={"col": c})

    def source_col(oy, oz):
        return col_of(lax.rem(my_y + SIDE - oy, SIDE), lax.rem(my_z + SIDE - oz, SIDE))

    def yz(cls, off):
        return off if cls == 0 else (off[1], off[0])

    def moved(off, dim, sign):
        new = list(off)
        new[dim] = (new[dim] + sign) % SIDE
        return tuple(new)

    def neighbour(cls, dim, sign):
        along_y = (dim == 0) == (cls == 0)
        y = lax.rem(my_y + SIDE + sign, SIDE) if along_y else my_y
        z = my_z if along_y else lax.rem(my_z + SIDE + sign, SIDE)
        return {"col": col_of(y, z)}

    def sem_at(cls, off, half):
        return cls * 32 + (off[0] * SIDE + off[1]) * 2 + (half or 0)

    def xz_region(cls, off, half):
        at = pl.ds(pl.multiple_of(source_col(*yz(cls, off)) * SLAB, SLAB), SLAB)
        full = x_full if cls == 0 else z_full
        if half is WHOLE:
            return full.at[:, at, :]
        return full.at[pl.ds(half * (OWNED // 2), OWNED // 2), at, :]

    def u_region(cls, off, half):
        oy, oz = yz(cls, off)
        buf = u_bufs[oy * SIDE + oz]
        if half is WHOLE:
            return buf.at[:, pl.ds(cls * CLASS_ROWS, CLASS_ROWS), :]
        return buf.at[:, pl.ds(cls * CLASS_ROWS + half * HALF_ROWS, HALF_ROWS), :]

    class Tree:
        def __init__(self, region, send_sems, recv_sems, same_place):
            self.region, self.send_sems, self.recv_sems = region, send_sems, recv_sems
            self.same_place, self.sent = same_place, []

        def copy(self, cls, off, dim, sign, half, source=None):
            there = moved(off, dim, sign)
            at = sem_at(cls, there, half)
            here = self.region(cls, off, half)
            copy = pltpu.make_async_remote_copy(
                src_ref=here if source is None else source,
                dst_ref=here if self.same_place else self.region(cls, there, half),
                send_sem=self.send_sems.at[at],
                recv_sem=self.recv_sems.at[at],
                device_id=neighbour(cls, dim, sign),
            )
            copy.start()
            self.sent.append(copy)

        def arrived(self, cls, off, half=WHOLE):
            at = sem_at(cls, off, half)
            here = self.region(cls, off, half)
            pltpu.make_async_remote_copy(
                src_ref=here, dst_ref=here,
                send_sem=self.send_sems.at[at], recv_sem=self.recv_sems.at[at],
                device_id=neighbour(cls, 0, 1),
            ).wait_recv()

        def first(self, sources=(None, None), dims=(0, 1)):
            for dim in dims:
                for sign in (1, -1):
                    for cls in (0, 1):
                        self.copy(cls, (0, 0), dim, sign, WHOLE, sources[cls])

        def near(self):
            self.spread()
            self.onward(0)

        def spread(self):
            for sign, off in ((1, 1), (-1, 3)):
                for cls in (0, 1):
                    self.arrived(cls, (off, 0))
                    self.copy(cls, (off, 0), 0, sign, 0 if sign > 0 else 1)
            for off in (1, 3):
                for cls in (0, 1):
                    for sign in (1, -1):
                        self.copy(cls, (off, 0), 1, sign, WHOLE)

        def onward(self, unit):
            for sign, off in ((1, 1), (-1, 3)):
                for cls in (0, 1):
                    self.arrived(cls, (unit, off))
                    self.copy(cls, (unit, off), 1, sign, 0 if sign > 0 else 1)

        def opposite(self):
            for cls in (0, 1):
                for half in (0, 1):
                    self.arrived(cls, (2, 0), half)
                for sign in (1, -1):
                    self.copy(cls, (2, 0), 1, sign, WHOLE)

        def last(self, unit):
            for cls in (0, 1):
                for half in (0, 1):
                    self.arrived(cls, (unit, 2), half)

        def drain(self):
            for copy in self.sent:
                copy.wait_send()

    xz = Tree(xz_region, xz_send, xz_recv, True)
    ut = Tree(u_region, u_send, u_recv, False)

    lane = lax.broadcasted_iota(i32, (1, C), 1)
    slots = [slot_ref[g] for g in range(GROUPS)]
    blocks = [lax.div(s, GMAX) for s in slots]
    owners = [lax.div(b, OWNED) for b in blocks]
    targets = []
    for g in range(GROUPS):
        earlier = sum([(owners[h] == owners[g]).astype(i32) for h in range(g)], jnp.int32(0))
        targets.append(owners[g] * PAIR + earlier)
    for copy in loads[:2]:
        copy.wait()
    for r in range(ROWS):
        note = jnp.zeros((1, C), i32)
        send_meta[r] = jnp.zeros((8, C), i32)
        for j in range(PAIR):
            t = r * PAIR + j
            src, code = jnp.int32(0), jnp.int32(0)
            for g in range(GROUPS):
                hit = targets[g] == t
                src = jnp.where(hit, g, src)
                code = jnp.where(hit, blocks[g] - owners[g] * OWNED + 1, code)
            note = jnp.where(lane == j, code, note)
            send_ut[r // 2, j, r % 2] = basis_ref[src].T
            rows = jnp.zeros((1, C), i32)
            for g in range(GROUPS):
                rows = jnp.where(jnp.full((1, C), targets[g]) == t, rows_ref[pl.ds(g, 1), :], rows)
            send_meta[r, pl.ds(j, 1), :] = rows
        send_meta[r, pl.ds(PAIR, 1), :] = note
    for j in range(PAIR):
        got_ut[my_row * PAIR + j] = send_ut[my_x, j, my_core]
    got_meta[my_row] = send_meta[my_row]

    pl.semaphore_wait(barrier, ROWS - 1 + 2 * (SIDE - 1))
    def exchange(d, r, sends, recvs):
        return pltpu.make_async_remote_copy(
            src_ref=send_meta.at[r], dst_ref=got_meta.at[my_row],
            send_sem=sends.at[d], recv_sem=recvs.at[d], device_id={"row": r},
        )

    def from_row(d, sends, recvs):
        r = lax.rem(my_row + ROWS - d, ROWS)
        return pltpu.make_async_remote_copy(
            src_ref=got_meta.at[r], dst_ref=got_meta.at[r],
            send_sem=sends.at[d], recv_sem=recvs.at[d], device_id={"row": r},
        )

    sides = [lax.rem(my_x + 1, SIDE), lax.rem(my_x + SIDE - 1, SIDE)]
    across = lax.rem(my_x + 2, SIDE)

    def to(source, dest, sem, x, core):
        return pltpu.make_async_remote_copy(
            src_ref=source, dst_ref=dest, send_sem=a_send.at[sem], recv_sem=a_recv.at[sem],
            device_id={"row": x * 2 + core},
        )

    def pair_of(row):
        return got_ut.at[pl.ds(row * PAIR, PAIR)]

    a_sent, m_sent, b_sent = [], [], []
    for i in range(2):
        a_sent.append(to(send_ut.at[across, i], relay.at[i], i, sides[i], my_core))
    for i in range(2):
        for same in range(2):
            core = lax.rem(my_core + same, 2)
            a_sent.append(to(send_ut.at[sides[i], :, core], pair_of(my_row), 2 + i * 2 + same, sides[i], core))
    other = lax.rem(my_core + 1, 2)
    a_sent.append(to(send_ut.at[my_x, :, other], pair_of(my_row), 6, my_x, other))

    for copy in a_sent[:2]:
        copy.start()
    for d, r in zip(range(1, ROWS), row_peers):
        m_sent.append(exchange(d, r, m_send, m_recv))
        m_sent[-1].start()
    for copy in loads[2:]:
        copy.wait()
    xz.first()
    for copy in a_sent[2:]:
        copy.start()

    xz.spread()
    for i in range(2):
        to(relay.at[i], relay.at[i], i, sides[i], my_core).wait_recv()
        origin = sides[1 - i] * 2 + my_core
        for core in range(2):
            a_sent.append(
                to(relay.at[i, core], got_ut.at[origin * PAIR + i], 7 + i * 4 + core * 2 + my_core, sides[i], core)
            )
            a_sent[-1].start()
    xz.onward(0)

    for d in range(1, ROWS):
        from_row(d, m_send, m_recv).wait_recv()
    note_copy = pltpu.make_async_copy(got_meta, small_got, local.at[4])
    note_copy.start()
    note_copy.wait()
    codes = [small_got[t // PAIR, PAIR, t % PAIR] for t in range(ROWS * PAIR)]
    picks = [jnp.int32(0)] * GROUPS
    kept = [jnp.int32(0)] * GROUPS
    count = jnp.int32(0)
    for t in range(ROWS * PAIR):
        for k in range(GROUPS):
            hit = (codes[t] > 0) & (count == k)
            picks[k] = jnp.where(hit, t, picks[k])
            kept[k] = jnp.where(hit, codes[t] - 1, kept[k])
        count = count + (codes[t] > 0).astype(i32)
    table = jnp.full((1, C), 16, i32)
    for k in range(GROUPS):
        table = jnp.where(lane == kept[k], k, table)
    for k in range(GROUPS):
        table = jnp.where(lane == GMAX + k, kept[k], table)
        block_ref[k] = kept[k]
    all_meta[my_col] = jnp.zeros((GMAX, C), i32)
    for k in range(GROUPS):
        rows = jnp.zeros((1, C), i32)
        for t in range(ROWS * PAIR):
            rows = jnp.where(jnp.full((1, C), picks[k]) == t, got_meta[t // PAIR, pl.ds(t % PAIR, 1), :], rows)
        all_meta[my_col, pl.ds(k, 1), :] = rows
    all_meta[my_col, pl.ds(GROUPS, 1), :] = table

    def noted(at, sem, c):
        return pltpu.make_async_remote_copy(
            src_ref=at, dst_ref=at,
            send_sem=b_send.at[sem], recv_sem=b_recv.at[sem], device_id={"col": c},
        )

    def notes_of(z):
        return all_meta.at[pl.ds(z * SIDE, SIDE)]

    for d in range(1, SIDE):
        b_sent.append(noted(all_meta.at[my_col], d, y_peers[d - 1]))
        b_sent[-1].start()
    xz.opposite()
    for d in range(1, SIDE):
        c = col_of(lax.rem(my_y + SIDE - d, SIDE), my_z)
        noted(all_meta.at[c], d, c).wait_recv()
    for d in range(1, SIDE):
        b_sent.append(noted(notes_of(my_z), SIDE + d, z_peers[d - 1]))
        b_sent[-1].start()
    xz.onward(1)
    xz.onward(3)

    for i in range(2):
        for same in range(2):
            core = lax.rem(my_core + same, 2)
            dest = pair_of(sides[1 - i] * 2 + core)
            to(dest, dest, 2 + i * 2 + same, sides[i], core).wait_recv()
    dest = pair_of(my_x * 2 + other)
    to(dest, dest, 6, my_x, other).wait_recv()
    for i in range(2):
        for core in range(2):
            dest = got_ut.at[(across * 2 + core) * PAIR + i]
            sem = 7 + i * 4 + my_core * 2 + core
            to(dest, dest, sem, sides[i], core).wait_recv()
    own = u_bufs[0]
    for k in range(GROUPS):
        own[k] = got_ut[picks[k]]

    ut.first(dims=(0,))
    xz.onward(2)
    ut.first(dims=(1,))

    down = lax.broadcasted_iota(i32, (N, C), 0)
    for k in range(GROUPS):
        q_all[k, :, :C] = own[k].T
        q_all[k, :, C:] = jnp.where(down == all_meta[my_col, pl.ds(k, 1), :], 1.0, 0.0).astype(bf16)

    for unit in range(SIDE):
        xz.last(unit)
    for d in range(1, SIDE):
        z = lax.rem(my_z + SIDE - d, SIDE)
        noted(notes_of(z), SIDE + d, col_of(my_y, z)).wait_recv()
    table_copy = pltpu.make_async_copy(all_meta.at[:, pl.ds(8, 8), :], small_all, local.at[5])
    table_copy.start()
    table_copy.wait()

    def places(k, cols):
        b = small_all[my_col, GROUPS - 8, GMAX + k]
        codes = [small_all[c, GROUPS - 8, b] for c in cols]
        return b, codes, [jnp.where(code < GROUPS, code, 0) for code in codes]

    def keep(k, c, code, tile):
        tiles_ref[k, pl.ds(pl.multiple_of(c * C, C), C), :] = jnp.where(
            jnp.full((C, C), code) < GROUPS, tile, 0.0
        )

    def per_group(work, unroll=UNROLL):
        def step(i, carry):
            for j in range(unroll):
                work(i * unroll + j)
            return carry

        lax.fori_loop(0, GROUPS // unroll, step, 0)

    def compute(batch):
        cols = [source_col(*off) for off in batch]
        bufs = [u_bufs[oy * SIDE + oz] for oy, oz in batch]

        def work(k):
            b, codes, at = places(k, cols)
            parts = [(buf[s], row_at(all_meta[c], s)) for buf, c, s in zip(bufs, cols, at)]
            for c, code, tile in zip(cols, codes, tiles_of(parts, x_full[b], z_full[b], q_all[k])):
                keep(k, c, code, tile)

        per_group(work)

    def compute_ahead():
        cols = [source_col(*off) for off in LATE]

        def work(k):
            b, _, at = places(k, cols)
            stack = jnp.concatenate(
                [one_hot_rows(row_at(all_meta[c], s)) for c, s in zip(cols, at)], axis=0
            )
            tx, tz = products_of(stack, x_full[b], z_full[b], q_all[k])
            for i in range(len(LATE)):
                ahead[k, i, :, :N] = tx[i * C : i * C + C]
                ahead[k, i, :, N:] = tz[i * C : i * C + C]

        per_group(work)

    def compute_late(first, last):
        cols = [source_col(*off) for off in LATE[first:last]]
        bufs = [u_bufs[oy * SIDE + oz] for oy, oz in LATE[first:last]]

        def work(k):
            b, codes, at = places(k, cols)
            stack = jnp.concatenate([buf[s] for buf, s in zip(bufs, at)], axis=0)
            tx, tz = products_of(stack, x_full[b], z_full[b], q_all[k])
            for i, (c, code) in enumerate(zip(cols, codes)):
                su0, se0 = tx[i * C : i * C + C, :C], tx[i * C : i * C + C, C:]
                su2, se2 = tz[i * C : i * C + C, :C], tz[i * C : i * C + C, C:]
                su1, se1, su3, se3 = [ahead[k, first + i, :, m * C : m * C + C] for m in range(4)]
                keep(k, c, code, su1 * se2 + se1 * su2 + su0 * se3 + se0 * su3)

        per_group(work, GROUPS)

    ut.near()
    compute_ahead()
    compute(BATCHES[0])
    ut.opposite()
    ut.onward(1)
    compute(BATCHES[1])
    ut.onward(3)
    compute(BATCHES[2])
    ut.last(0)
    compute(BATCHES[3])
    ut.onward(2)
    ut.last(1)
    compute_late(0, 2)
    ut.last(3)
    compute_late(2, 4)
    ut.last(2)
    compute_late(4, 5)

    xz.drain()
    ut.drain()
    for copy in a_sent + m_sent + b_sent:
        copy.wait_send()


def place_kernel(block_ref, tiles_ref, out_ref, zeros, full_sem, zero_sem):
    zeros[...] = jnp.zeros_like(zeros)
    full = [
        pltpu.make_async_copy(tiles_ref.at[k], out_ref.at[block_ref[k]], full_sem.at[k])
        for k in range(GROUPS)
    ]
    for copy in full:
        copy.start()
    count = jnp.int32(0)
    absent = [jnp.int32(0)] * (OWNED - GROUPS)
    for b in range(OWNED):
        found = block_ref[0] == b
        for k in range(1, GROUPS):
            found = found | (block_ref[k] == b)
        for m in range(OWNED - GROUPS):
            absent[m] = jnp.where(jnp.logical_not(found) & (count == m), b, absent[m])
        count = count + jnp.where(found, 0, 1)
    empty = [
        pltpu.make_async_copy(zeros, out_ref.at[absent[m]], zero_sem.at[m])
        for m in range(OWNED - GROUPS)
    ]
    for copy in empty:
        copy.start()
    for copy in full + empty:
        copy.wait()


def body(basis, row_index, group_slot, x_blocks, zinv_blocks):
    hbm, vmem, smem, anywhere = (
        pl.BlockSpec(memory_space=pltpu.HBM),
        pl.BlockSpec(memory_space=pltpu.VMEM),
        pl.BlockSpec(memory_space=pltpu.SMEM),
        pl.BlockSpec(memory_space=pl.ANY),
    )
    dma = pltpu.SemaphoreType.DMA
    tiles, blocks = pl.pallas_call(
        gather_kernel,
        out_shape=(
            pltpu.VMEM((GROUPS, GMAX * C, C), f32),
            jax.ShapeDtypeStruct((GMAX,), i32),
        ),
        in_specs=[smem, hbm, hbm, hbm, hbm],
        out_specs=(vmem, smem),
        scratch_shapes=[
            pltpu.VMEM((GROUPS, N, C), bf16),
            pltpu.VMEM((GROUPS, C), i32),
            pltpu.VMEM((SIDE, PAIR, 2, C, N), bf16),
            pltpu.VMEM((2, 2, C, N), bf16),
            pltpu.VMEM((ROWS * PAIR, C, N), bf16),
            pltpu.VMEM((ROWS, 8, C), i32),
            pltpu.VMEM((ROWS, 8, C), i32),
            pltpu.VMEM((COLS, GMAX, C), i32),
            pltpu.SMEM((ROWS, 8, C), i32),
            pltpu.SMEM((COLS, 8, C), i32),
            pltpu.VMEM((OWNED, N, N), bf16),
            pltpu.VMEM((OWNED, N, N), bf16),
            pltpu.VMEM((GROUPS, N, N), bf16),
            pltpu.VMEM((GROUPS, len(LATE), C, 2 * N), f32),
        ]
        + [pltpu.VMEM((GROUPS, C, N), bf16)] * 16
        + [dma((64,))] * 4
        + [dma((16,))] * 2
        + [dma((ROWS,))] * 2
        + [dma((2 * SIDE,))] * 2
        + [dma((6,))],
        compiler_params=pltpu.CompilerParams(
            collective_id=0, has_side_effects=True, vmem_limit_bytes=57_500_000
        ),
        name="gather_tiles",
    )(group_slot, basis, row_index, x_blocks, zinv_blocks)
    return pl.pallas_call(
        place_kernel,
        out_shape=jax.ShapeDtypeStruct((OWNED, GMAX * C, C), f32),
        in_specs=[smem, vmem],
        out_specs=anywhere,
        scratch_shapes=[pltpu.VMEM((GMAX * C, C), f32), dma((GROUPS,)), dma((OWNED - GROUPS,))],
        compiler_params=pltpu.CompilerParams(vmem_limit_bytes=16 << 20),
        name="place_tiles",
    )(blocks, tiles)


def solution(mesh):
    placed = (
        P(("row", "col"), None, None),
        P(("row", "col"), None),
        P(("row", "col")),
        P("row", "col", None),
        P("row", "col", None),
    )
    return jax.shard_map(
        body, mesh=mesh, in_specs=placed, out_specs=P("row", None, "col"), check_vma=False
    )
```

```python
import jax
import jax.numpy as jnp
from jax import lax
from jax.experimental import pallas as pl
from jax.experimental.pallas import tpu as pltpu
from jax.sharding import PartitionSpec as P

bf16, f32, i32 = jnp.bfloat16, jnp.float32, jnp.int32
N, C, GMAX = 256, 128, 16
ROWS, COLS, SIDE = 8, 16, 4
OWNED, GROUPS, PAIR = 12, 9, 2
SLAB = N // COLS
CLASS_ROWS = C // 2
HALF_ROWS = CLASS_ROWS // 2
WHOLE = None
BATCHES = (
    ((0, 0), (1, 0), (3, 0), (0, 1)),
    ((0, 3), (1, 1)),
    ((1, 3), (3, 1), (3, 3)),
    ((2, 0), (0, 2)),
)
LATE = ((2, 1), (1, 2), (2, 3), (3, 2), (2, 2))
UNROLL = 3


def col_of(y, z):
    return z * SIDE + y


def one_hot_rows(rows):
    column = jnp.broadcast_to(rows, (C, C)).T
    lanes = lax.broadcasted_iota(i32, (C, C), 1)
    both = jnp.concatenate([column == lanes, column == lanes + C], axis=1)
    return jnp.where(both, 1.0, 0.0).astype(bf16)


def row_at(table, at):
    down = lax.broadcasted_iota(i32, table.shape, 0)
    return jnp.sum(jnp.where(down == at, table, 0), axis=0, keepdims=True)


def tiles_of(parts, x, z, q):
    stack = jnp.concatenate([a for ut, rows in parts for a in (ut, one_hot_rows(rows))], axis=0)
    tx, tz = products_of(stack, x, z, q)
    out = []
    for i in range(len(parts)):
        lo, mid, hi = 2 * C * i, 2 * C * i + C, 2 * C * i + 2 * C
        su0, se0, su1, se1 = tx[lo:mid, :C], tx[lo:mid, C:], tx[mid:hi, :C], tx[mid:hi, C:]
        su2, se2, su3, se3 = tz[lo:mid, :C], tz[lo:mid, C:], tz[mid:hi, :C], tz[mid:hi, C:]
        out.append(su1 * se2 + se1 * su2 + su0 * se3 + se0 * su3)
    return out


def products_of(stack, x, z, q):
    sx = jnp.dot(stack, x, preferred_element_type=f32).astype(bf16)
    sz = jnp.dot(stack, z, preferred_element_type=f32).astype(bf16)
    return (
        jnp.dot(sx, q, preferred_element_type=f32),
        jnp.dot(sz, q, preferred_element_type=f32),
    )


def gather_kernel(
    slot_ref, basis_hbm, rows_hbm, x_ref, z_ref, tiles_ref, block_ref,
    basis_ref, rows_ref, send_ut, relay, got_ut, send_meta, got_meta, all_meta, small_got, small_all,
    x_full, z_full, q_all, ahead, *rest,
):
    u_bufs = rest[:16]
    (xz_send, xz_recv, u_send, u_recv, a_send, a_recv, m_send, m_recv, b_send, b_recv, local) = rest[16:]
    my_row, my_col = lax.axis_index("row"), lax.axis_index("col")
    my_y, my_z = lax.rem(my_col, SIDE), my_col // SIDE
    my_x, my_core = my_row // 2, lax.rem(my_row, 2)
    mine = pl.ds(pl.multiple_of(my_col * SLAB, SLAB), SLAB)
    loads = [
        pltpu.make_async_copy(source, dest, local.at[i])
        for i, (source, dest) in enumerate((
            (basis_hbm, basis_ref),
            (rows_hbm, rows_ref),
            (x_ref, x_full.at[:, mine, :]),
            (z_ref, z_full.at[:, mine, :]),
        ))
    ]
    for copy in loads:
        copy.start()

    row_peers = [lax.rem(my_row + d, ROWS) for d in range(1, ROWS)]
    y_peers = [col_of(lax.rem(my_y + d, SIDE), my_z) for d in range(1, SIDE)]
    z_peers = [col_of(my_y, lax.rem(my_z + d, SIDE)) for d in range(1, SIDE)]
    barrier = pltpu.get_barrier_semaphore()
    for r in row_peers:
        pl.semaphore_signal(barrier, inc=1, device_id={"row": r})
    for c in y_peers + z_peers:
        pl.semaphore_signal(barrier, inc=1, device_id={"col": c})

    def source_col(oy, oz):
        return col_of(lax.rem(my_y + SIDE - oy, SIDE), lax.rem(my_z + SIDE - oz, SIDE))

    def yz(cls, off):
        return off if cls == 0 else (off[1], off[0])

    def moved(off, dim, sign):
        new = list(off)
        new[dim] = (new[dim] + sign) % SIDE
        return tuple(new)

    def neighbour(cls, dim, sign):
        along_y = (dim == 0) == (cls == 0)
        y = lax.rem(my_y + SIDE + sign, SIDE) if along_y else my_y
        z = my_z if along_y else lax.rem(my_z + SIDE + sign, SIDE)
        return {"col": col_of(y, z)}

    def sem_at(cls, off, half):
        return cls * 32 + (off[0] * SIDE + off[1]) * 2 + (half or 0)

    def xz_region(cls, off, half):
        at = pl.ds(pl.multiple_of(source_col(*yz(cls, off)) * SLAB, SLAB), SLAB)
        full = x_full if cls == 0 else z_full
        if half is WHOLE:
            return full.at[:, at, :]
        return full.at[pl.ds(half * (OWNED // 2), OWNED // 2), at, :]

    def u_region(cls, off, half):
        oy, oz = yz(cls, off)
        buf = u_bufs[oy * SIDE + oz]
        if half is WHOLE:
            return buf.at[:, pl.ds(cls * CLASS_ROWS, CLASS_ROWS), :]
        return buf.at[:, pl.ds(cls * CLASS_ROWS + half * HALF_ROWS, HALF_ROWS), :]

    class Tree:
        def __init__(self, region, send_sems, recv_sems, same_place):
            self.region, self.send_sems, self.recv_sems = region, send_sems, recv_sems
            self.same_place, self.sent = same_place, []

        def copy(self, cls, off, dim, sign, half, source=None):
            there = moved(off, dim, sign)
            at = sem_at(cls, there, half)
            here = self.region(cls, off, half)
            copy = pltpu.make_async_remote_copy(
                src_ref=here if source is None else source,
                dst_ref=here if self.same_place else self.region(cls, there, half),
                send_sem=self.send_sems.at[at],
                recv_sem=self.recv_sems.at[at],
                device_id=neighbour(cls, dim, sign),
            )
            copy.start()
            self.sent.append(copy)

        def arrived(self, cls, off, half=WHOLE):
            at = sem_at(cls, off, half)
            here = self.region(cls, off, half)
            pltpu.make_async_remote_copy(
                src_ref=here, dst_ref=here,
                send_sem=self.send_sems.at[at], recv_sem=self.recv_sems.at[at],
                device_id=neighbour(cls, 0, 1),
            ).wait_recv()

        def first(self, sources=(None, None), dims=(0, 1)):
            for dim in dims:
                for sign in (1, -1):
                    for cls in (0, 1):
                        self.copy(cls, (0, 0), dim, sign, WHOLE, sources[cls])

        def near(self):
            self.spread()
            self.onward(0)

        def spread(self):
            for sign, off in ((1, 1), (-1, 3)):
                for cls in (0, 1):
                    self.arrived(cls, (off, 0))
                    self.copy(cls, (off, 0), 0, sign, 0 if sign > 0 else 1)
            for off in (1, 3):
                for cls in (0, 1):
                    for sign in (1, -1):
                        self.copy(cls, (off, 0), 1, sign, WHOLE)

        def onward(self, unit):
            for sign, off in ((1, 1), (-1, 3)):
                for cls in (0, 1):
                    self.arrived(cls, (unit, off))
                    self.copy(cls, (unit, off), 1, sign, 0 if sign > 0 else 1)

        def opposite(self):
            for cls in (0, 1):
                for half in (0, 1):
                    self.arrived(cls, (2, 0), half)
                for sign in (1, -1):
                    self.copy(cls, (2, 0), 1, sign, WHOLE)

        def last(self, unit):
            for cls in (0, 1):
                for half in (0, 1):
                    self.arrived(cls, (unit, 2), half)

        def drain(self):
            for copy in self.sent:
                copy.wait_send()

    xz = Tree(xz_region, xz_send, xz_recv, True)
    ut = Tree(u_region, u_send, u_recv, False)

    lane = lax.broadcasted_iota(i32, (1, C), 1)
    slots = [slot_ref[g] for g in range(GROUPS)]
    blocks = [lax.div(s, GMAX) for s in slots]
    owners = [lax.div(b, OWNED) for b in blocks]
    targets = []
    for g in range(GROUPS):
        earlier = sum([(owners[h] == owners[g]).astype(i32) for h in range(g)], jnp.int32(0))
        targets.append(owners[g] * PAIR + earlier)
    for copy in loads[:2]:
        copy.wait()
    for r in range(ROWS):
        note = jnp.zeros((1, C), i32)
        send_meta[r] = jnp.zeros((8, C), i32)
        for j in range(PAIR):
            t = r * PAIR + j
            src, code = jnp.int32(0), jnp.int32(0)
            for g in range(GROUPS):
                hit = targets[g] == t
                src = jnp.where(hit, g, src)
                code = jnp.where(hit, blocks[g] - owners[g] * OWNED + 1, code)
            note = jnp.where(lane == j, code, note)
            send_ut[r // 2, j, r % 2] = basis_ref[src].T
            rows = jnp.zeros((1, C), i32)
            for g in range(GROUPS):
                rows = jnp.where(jnp.full((1, C), targets[g]) == t, rows_ref[pl.ds(g, 1), :], rows)
            send_meta[r, pl.ds(j, 1), :] = rows
        send_meta[r, pl.ds(PAIR, 1), :] = note
    for j in range(PAIR):
        got_ut[my_row * PAIR + j] = send_ut[my_x, j, my_core]
    got_meta[my_row] = send_meta[my_row]

    pl.semaphore_wait(barrier, ROWS - 1 + 2 * (SIDE - 1))
    def exchange(d, r, sends, recvs):
        return pltpu.make_async_remote_copy(
            src_ref=send_meta.at[r], dst_ref=got_meta.at[my_row],
            send_sem=sends.at[d], recv_sem=recvs.at[d], device_id={"row": r},
        )

    def from_row(d, sends, recvs):
        r = lax.rem(my_row + ROWS - d, ROWS)
        return pltpu.make_async_remote_copy(
            src_ref=got_meta.at[r], dst_ref=got_meta.at[r],
            send_sem=sends.at[d], recv_sem=recvs.at[d], device_id={"row": r},
        )

    sides = [lax.rem(my_x + 1, SIDE), lax.rem(my_x + SIDE - 1, SIDE)]
    across = lax.rem(my_x + 2, SIDE)

    def to(source, dest, sem, x, core):
        return pltpu.make_async_remote_copy(
            src_ref=source, dst_ref=dest, send_sem=a_send.at[sem], recv_sem=a_recv.at[sem],
            device_id={"row": x * 2 + core},
        )

    def pair_of(row):
        return got_ut.at[pl.ds(row * PAIR, PAIR)]

    a_sent, m_sent, b_sent = [], [], []
    for i in range(2):
        a_sent.append(to(send_ut.at[across, i], relay.at[i], i, sides[i], my_core))
    for i in range(2):
        for same in range(2):
            core = lax.rem(my_core + same, 2)
            a_sent.append(to(send_ut.at[sides[i], :, core], pair_of(my_row), 2 + i * 2 + same, sides[i], core))
    other = lax.rem(my_core + 1, 2)
    a_sent.append(to(send_ut.at[my_x, :, other], pair_of(my_row), 6, my_x, other))

    for copy in a_sent[:2]:
        copy.start()
    for d, r in zip(range(1, ROWS), row_peers):
        m_sent.append(exchange(d, r, m_send, m_recv))
        m_sent[-1].start()
    for copy in loads[2:]:
        copy.wait()
    xz.first()
    for copy in a_sent[2:]:
        copy.start()

    xz.spread()
    for i in range(2):
        to(relay.at[i], relay.at[i], i, sides[i], my_core).wait_recv()
        origin = sides[1 - i] * 2 + my_core
        for core in range(2):
            a_sent.append(
                to(relay.at[i, core], got_ut.at[origin * PAIR + i], 7 + i * 4 + core * 2 + my_core, sides[i], core)
            )
            a_sent[-1].start()
    xz.onward(0)

    for d in range(1, ROWS):
        from_row(d, m_send, m_recv).wait_recv()
    note_copy = pltpu.make_async_copy(got_meta, small_got, local.at[4])
    note_copy.start()
    note_copy.wait()
    codes = [small_got[t // PAIR, PAIR, t % PAIR] for t in range(ROWS * PAIR)]
    picks = [jnp.int32(0)] * GROUPS
    kept = [jnp.int32(0)] * GROUPS
    count = jnp.int32(0)
    for t in range(ROWS * PAIR):
        for k in range(GROUPS):
            hit = (codes[t] > 0) & (count == k)
            picks[k] = jnp.where(hit, t, picks[k])
            kept[k] = jnp.where(hit, codes[t] - 1, kept[k])
        count = count + (codes[t] > 0).astype(i32)
    table = jnp.full((1, C), 16, i32)
    for k in range(GROUPS):
        table = jnp.where(lane == kept[k], k, table)
    for k in range(GROUPS):
        table = jnp.where(lane == GMAX + k, kept[k], table)
    block_ref[...] = jnp.broadcast_to(table, block_ref.shape)
    all_meta[my_col] = jnp.zeros((GMAX, C), i32)
    for k in range(GROUPS):
        rows = jnp.zeros((1, C), i32)
        for t in range(ROWS * PAIR):
            rows = jnp.where(jnp.full((1, C), picks[k]) == t, got_meta[t // PAIR, pl.ds(t % PAIR, 1), :], rows)
        all_meta[my_col, pl.ds(k, 1), :] = rows
    all_meta[my_col, pl.ds(GROUPS, 1), :] = table

    def noted(at, sem, c):
        return pltpu.make_async_remote_copy(
            src_ref=at, dst_ref=at,
            send_sem=b_send.at[sem], recv_sem=b_recv.at[sem], device_id={"col": c},
        )

    def notes_of(z):
        return all_meta.at[pl.ds(z * SIDE, SIDE)]

    for d in range(1, SIDE):
        b_sent.append(noted(all_meta.at[my_col], d, y_peers[d - 1]))
        b_sent[-1].start()
    xz.opposite()
    for d in range(1, SIDE):
        c = col_of(lax.rem(my_y + SIDE - d, SIDE), my_z)
        noted(all_meta.at[c], d, c).wait_recv()
    for d in range(1, SIDE):
        b_sent.append(noted(notes_of(my_z), SIDE + d, z_peers[d - 1]))
        b_sent[-1].start()
    xz.onward(1)
    xz.onward(3)

    for i in range(2):
        for same in range(2):
            core = lax.rem(my_core + same, 2)
            dest = pair_of(sides[1 - i] * 2 + core)
            to(dest, dest, 2 + i * 2 + same, sides[i], core).wait_recv()
    dest = pair_of(my_x * 2 + other)
    to(dest, dest, 6, my_x, other).wait_recv()
    for i in range(2):
        for core in range(2):
            dest = got_ut.at[(across * 2 + core) * PAIR + i]
            sem = 7 + i * 4 + my_core * 2 + core
            to(dest, dest, sem, sides[i], core).wait_recv()
    own = u_bufs[0]
    for k in range(GROUPS):
        own[k] = got_ut[picks[k]]

    ut.first(dims=(0,))
    xz.onward(2)
    ut.first(dims=(1,))

    down = lax.broadcasted_iota(i32, (N, C), 0)
    for k in range(GROUPS):
        q_all[k, :, :C] = own[k].T
        q_all[k, :, C:] = jnp.where(down == all_meta[my_col, pl.ds(k, 1), :], 1.0, 0.0).astype(bf16)

    for unit in range(SIDE):
        xz.last(unit)
    for d in range(1, SIDE):
        z = lax.rem(my_z + SIDE - d, SIDE)
        noted(notes_of(z), SIDE + d, col_of(my_y, z)).wait_recv()
    table_copy = pltpu.make_async_copy(all_meta.at[:, pl.ds(8, 8), :], small_all, local.at[5])
    table_copy.start()
    table_copy.wait()

    def places(k, cols):
        b = small_all[my_col, GROUPS - 8, GMAX + k]
        codes = [small_all[c, GROUPS - 8, b] for c in cols]
        return b, codes, [jnp.where(code < GROUPS, code, 0) for code in codes]

    def keep(k, c, code, tile):
        tiles_ref[k, pl.ds(pl.multiple_of(c * C, C), C), :] = jnp.where(
            jnp.full((C, C), code) < GROUPS, tile, 0.0
        )

    def per_group(work, unroll=UNROLL):
        def step(i, carry):
            for j in range(unroll):
                work(i * unroll + j)
            return carry

        lax.fori_loop(0, GROUPS // unroll, step, 0)

    def compute(batch):
        cols = [source_col(*off) for off in batch]
        bufs = [u_bufs[oy * SIDE + oz] for oy, oz in batch]

        def work(k):
            b, codes, at = places(k, cols)
            parts = [(buf[s], row_at(all_meta[c], s)) for buf, c, s in zip(bufs, cols, at)]
            for c, code, tile in zip(cols, codes, tiles_of(parts, x_full[b], z_full[b], q_all[k])):
                keep(k, c, code, tile)

        per_group(work)

    def compute_ahead():
        cols = [source_col(*off) for off in LATE]

        def work(k):
            b, _, at = places(k, cols)
            stack = jnp.concatenate(
                [one_hot_rows(row_at(all_meta[c], s)) for c, s in zip(cols, at)], axis=0
            )
            tx, tz = products_of(stack, x_full[b], z_full[b], q_all[k])
            for i in range(len(LATE)):
                ahead[k, i, :, :N] = tx[i * C : i * C + C]
                ahead[k, i, :, N:] = tz[i * C : i * C + C]

        per_group(work)

    def compute_late(first, last):
        cols = [source_col(*off) for off in LATE[first:last]]
        bufs = [u_bufs[oy * SIDE + oz] for oy, oz in LATE[first:last]]

        def work(k):
            b, codes, at = places(k, cols)
            stack = jnp.concatenate([buf[s] for buf, s in zip(bufs, at)], axis=0)
            tx, tz = products_of(stack, x_full[b], z_full[b], q_all[k])
            for i, (c, code) in enumerate(zip(cols, codes)):
                su0, se0 = tx[i * C : i * C + C, :C], tx[i * C : i * C + C, C:]
                su2, se2 = tz[i * C : i * C + C, :C], tz[i * C : i * C + C, C:]
                su1, se1, su3, se3 = [ahead[k, first + i, :, m * C : m * C + C] for m in range(4)]
                keep(k, c, code, su1 * se2 + se1 * su2 + su0 * se3 + se0 * su3)

        per_group(work, GROUPS)

    ut.near()
    compute_ahead()
    compute(BATCHES[0])
    ut.opposite()
    ut.onward(1)
    compute(BATCHES[1])
    ut.onward(3)
    compute(BATCHES[2])
    ut.last(0)
    compute(BATCHES[3])
    ut.onward(2)
    ut.last(1)
    compute_late(0, 2)
    ut.last(3)
    compute_late(2, 4)
    ut.last(2)
    compute_late(4, 5)

    xz.drain()
    ut.drain()
    for copy in a_sent + m_sent + b_sent:
        copy.wait_send()


def place_kernel(table_ref, tiles_ref, out_ref, zeros, table, full_sem, zero_sem, table_sem):
    table_copy = pltpu.make_async_copy(table_ref, table, table_sem)
    table_copy.start()
    zeros[...] = jnp.zeros_like(zeros)
    table_copy.wait()
    block_ref = [table[0, GMAX + k] for k in range(GROUPS)]
    full = [
        pltpu.make_async_copy(tiles_ref.at[k], out_ref.at[block_ref[k]], full_sem.at[k])
        for k in range(GROUPS)
    ]
    for copy in full:
        copy.start()
    count = jnp.int32(0)
    absent = [jnp.int32(0)] * (OWNED - GROUPS)
    for b in range(OWNED):
        found = block_ref[0] == b
        for k in range(1, GROUPS):
            found = found | (block_ref[k] == b)
        for m in range(OWNED - GROUPS):
            absent[m] = jnp.where(jnp.logical_not(found) & (count == m), b, absent[m])
        count = count + jnp.where(found, 0, 1)
    empty = [
        pltpu.make_async_copy(zeros, out_ref.at[absent[m]], zero_sem.at[m])
        for m in range(OWNED - GROUPS)
    ]
    for copy in empty:
        copy.start()
    for copy in full + empty:
        copy.wait()


def body(basis, row_index, group_slot, x_blocks, zinv_blocks):
    hbm, vmem, smem, anywhere = (
        pl.BlockSpec(memory_space=pltpu.HBM),
        pl.BlockSpec(memory_space=pltpu.VMEM),
        pl.BlockSpec(memory_space=pltpu.SMEM),
        pl.BlockSpec(memory_space=pl.ANY),
    )
    dma = pltpu.SemaphoreType.DMA
    tiles, blocks = pl.pallas_call(
        gather_kernel,
        out_shape=(
            pltpu.VMEM((GROUPS, GMAX * C, C), f32),
            pltpu.VMEM((8, C), i32),
        ),
        in_specs=[smem, hbm, hbm, hbm, hbm],
        out_specs=(vmem, vmem),
        scratch_shapes=[
            pltpu.VMEM((GROUPS, N, C), bf16),
            pltpu.VMEM((GROUPS, C), i32),
            pltpu.VMEM((SIDE, PAIR, 2, C, N), bf16),
            pltpu.VMEM((2, 2, C, N), bf16),
            pltpu.VMEM((ROWS * PAIR, C, N), bf16),
            pltpu.VMEM((ROWS, 8, C), i32),
            pltpu.VMEM((ROWS, 8, C), i32),
            pltpu.VMEM((COLS, GMAX, C), i32),
            pltpu.SMEM((ROWS, 8, C), i32),
            pltpu.SMEM((COLS, 8, C), i32),
            pltpu.VMEM((OWNED, N, N), bf16),
            pltpu.VMEM((OWNED, N, N), bf16),
            pltpu.VMEM((GROUPS, N, N), bf16),
            pltpu.VMEM((GROUPS, len(LATE), C, 2 * N), f32),
        ]
        + [pltpu.VMEM((GROUPS, C, N), bf16)] * 16
        + [dma((64,))] * 4
        + [dma((16,))] * 2
        + [dma((ROWS,))] * 2
        + [dma((2 * SIDE,))] * 2
        + [dma((6,))],
        compiler_params=pltpu.CompilerParams(
            collective_id=0, has_side_effects=True, vmem_limit_bytes=57_500_000
        ),
        name="gather_tiles",
    )(group_slot, basis, row_index, x_blocks, zinv_blocks)
    return pl.pallas_call(
        place_kernel,
        out_shape=jax.ShapeDtypeStruct((OWNED, GMAX * C, C), f32),
        in_specs=[vmem, vmem],
        out_specs=anywhere,
        scratch_shapes=[pltpu.VMEM((GMAX * C, C), f32), pltpu.SMEM((8, C), i32), dma((GROUPS,)), dma((OWNED - GROUPS,)), dma],
        compiler_params=pltpu.CompilerParams(vmem_limit_bytes=16 << 20),
        name="place_tiles",
    )(blocks, tiles)


def solution(mesh):
    placed = (
        P(("row", "col"), None, None),
        P(("row", "col"), None),
        P(("row", "col")),
        P("row", "col", None),
        P("row", "col", None),
    )
    return jax.shard_map(
        body, mesh=mesh, in_specs=placed, out_specs=P("row", None, "col"), check_vma=False
    )
```
